8 devices in a mesh: dp: 2 (over z, y), ep: 4 (over x, core).
Axes of the slice: x: 2, y: 2, z: 1, core: 2. Of those that a mesh axis runs over, the one named last changes fastest.
Arguments:
- x_in: bfloat16 [16384, 1536], P(('dp', 'ep'))
- dy_in: bfloat16 [16384, 1536], P(('dp', 'ep'))
- top_ids: int32 [16384, 6], P(('dp', 'ep'))
- w_router: bfloat16 [1536, 64], P(('dp', 'ep'))
- w_gate: bfloat16 [64, 1536, 512], P('ep', 'dp')
- w_up: bfloat16 [64, 1536, 512], P('ep', 'dp')
- w_down: bfloat16 [64, 512, 1536], P('ep', 'dp')
- s_gate: bfloat16 [1536, 1024], P(('dp', 'ep'))
- s_up: bfloat16 [1536, 1024], P(('dp', 'ep'))
- s_down: bfloat16 [1024, 1536], P(('dp', 'ep'))
Outputs:
- output 1: bfloat16 [16384, 1536], P(('dp', 'ep'))
- output 2: bfloat16 [16384, 1536], P(('dp', 'ep'))
- output 3: float32 [1536, 64], P(('dp', 'ep'))
- output 4: float32 [64, 1536, 512], P('ep', 'dp')
- output 5: float32 [64, 1536, 512], P('ep', 'dp')
- output 6: float32 [64, 512, 1536], P('ep', 'dp')
- output 7: float32 [1536, 1024], P(('dp', 'ep'))
- output 8: float32 [1536, 1024], P(('dp', 'ep'))
- output 9: float32 [1024, 1536], P(('dp', 'ep'))
All inputs are finite; a program needn't handle non-finite values.
Results may differ from the reference program's by a relative error of at most 0.00497808.
Values are sent between devices in bfloat16 or wider.
A program may use at most 1 GiB of HBM per device.

```python
import math
import jax
import jax.numpy as jnp
from jax import lax

MODEL_DIM = 1536
NUM_EXPERTS = 64
TOP_K = 6
EXPERT_FF = 512
SHARED_FF = 1024
TOK_DEV = 2048
NUM_BLOCKS = 8
SLOT_CAP = 2 * TOK_DEV * TOP_K // NUM_EXPERTS
TOKENS = TOK_DEV * NUM_BLOCKS


def draw_routes(route_key):
    choices = TOK_DEV * TOP_K
    rank_expert = jax.random.permutation(jax.random.fold_in(route_key, 1), NUM_EXPERTS)
    rank_ids = jnp.arange(1, NUM_EXPERTS, dtype=jnp.int32)
    weights = 16384 // (rank_ids + NUM_EXPERTS // 2)
    spare_cnt = choices - SLOT_CAP - (NUM_EXPERTS - 1)
    base_cnt = 1 + (spare_cnt * weights) // jnp.sum(weights)
    short_cnt = spare_cnt - jnp.sum(base_cnt - 1)
    tail_cnt = base_cnt + (rank_ids >= NUM_EXPERTS - short_cnt).astype(jnp.int32)
    counts = jnp.concatenate([jnp.full((1,), SLOT_CAP, dtype=jnp.int32), tail_cnt])
    run_ends = jnp.cumsum(counts)
    slot_rank = jnp.searchsorted(run_ends, jnp.arange(choices, dtype=jnp.int32), side='right')
    id_grid = rank_expert[slot_rank].reshape(TOP_K, TOK_DEV).T
    blk_keys = jax.random.split(jax.random.fold_in(route_key, 2), NUM_BLOCKS)
    blocks = jax.vmap(lambda blk_key: id_grid[jax.random.permutation(blk_key, TOK_DEV)])(blk_keys)
    return blocks.reshape(TOKENS, TOP_K).astype(jnp.int32)


def setup_inputs(seed: int = 0) -> dict:
    sub_keys = jax.random.split(jax.random.key(seed), 11)
    top_ids = draw_routes(sub_keys[0])
    w_router = (jax.random.normal(sub_keys[1], (MODEL_DIM, NUM_EXPERTS), jnp.float32) * MODEL_DIM ** -0.5).astype(jnp.bfloat16)
    strength = jax.random.uniform(sub_keys[2], (TOKENS, TOP_K), jnp.float32, 0.6, 1.1) * math.log(NUM_EXPERTS)
    picked = (top_ids[:, :, None] == jnp.arange(NUM_EXPERTS)[None, None, :]).astype(jnp.float32)
    coeffs = jnp.einsum('tk,tke->te', strength, picked)
    noise_val = jax.random.normal(sub_keys[3], (TOKENS, MODEL_DIM), jnp.float32)
    x_in = (noise_val + jnp.dot(coeffs, w_router.astype(jnp.float32).T)).astype(jnp.bfloat16)
    dy_in = jax.random.normal(sub_keys[4], (TOKENS, MODEL_DIM), jnp.float32).astype(jnp.bfloat16)
    w_gate = (jax.random.normal(sub_keys[5], (NUM_EXPERTS, MODEL_DIM, EXPERT_FF), jnp.float32) * MODEL_DIM ** -0.5).astype(jnp.bfloat16)
    w_up = (jax.random.normal(sub_keys[6], (NUM_EXPERTS, MODEL_DIM, EXPERT_FF), jnp.float32) * MODEL_DIM ** -0.5).astype(jnp.bfloat16)
    w_down = (jax.random.normal(sub_keys[7], (NUM_EXPERTS, EXPERT_FF, MODEL_DIM), jnp.float32) * EXPERT_FF ** -0.5).astype(jnp.bfloat16)
    s_gate = (jax.random.normal(sub_keys[8], (MODEL_DIM, SHARED_FF), jnp.float32) * MODEL_DIM ** -0.5).astype(jnp.bfloat16)
    s_up = (jax.random.normal(sub_keys[9], (MODEL_DIM, SHARED_FF), jnp.float32) * MODEL_DIM ** -0.5).astype(jnp.bfloat16)
    s_down = (jax.random.normal(sub_keys[10], (SHARED_FF, MODEL_DIM), jnp.float32) * (0.5 * SHARED_FF ** -0.5)).astype(jnp.bfloat16)
    return {'x_in': x_in, 'dy_in': dy_in, 'top_ids': top_ids, 'w_router': w_router, 'w_gate': w_gate, 'w_up': w_up, 'w_down': w_down, 's_gate': s_gate, 's_up': s_up, 's_down': s_down}


def slot_tables(top_blk):
    flat_ids = top_blk.reshape(-1)
    sort_order = jnp.argsort(flat_ids, stable=True)
    counts = jnp.bincount(flat_ids, length=NUM_EXPERTS)
    starts = jnp.cumsum(counts) - counts
    slot_idx = jnp.arange(SLOT_CAP)
    is_valid = slot_idx[None, :] < counts[:, None]
    assign = sort_order[jnp.minimum(starts[:, None] + slot_idx[None, :], TOK_DEV * TOP_K - 1)]
    inverse = jnp.argsort(sort_order, stable=True)
    slot_pos = flat_ids * SLOT_CAP + inverse - starts[flat_ids]
    return assign, is_valid, slot_pos


def silu_grads(d_hidden, gate_pre, up_pre):
    sig_gate = jax.nn.sigmoid(gate_pre)
    silu_gate = gate_pre * sig_gate
    d_gate = (d_hidden * up_pre * sig_gate * (1.0 + gate_pre * (1.0 - sig_gate))).astype(jnp.bfloat16)
    d_up = (d_hidden * silu_gate).astype(jnp.bfloat16)
    return d_gate, d_up


def reference(x_in, dy_in, top_ids, w_router, w_gate, w_up, w_down, s_gate, s_up, s_down):
    logits = jnp.dot(x_in, w_router, preferred_element_type=jnp.float32)
    router_prob = jax.nn.softmax(logits, axis=-1)
    picked = (top_ids[:, :, None] == jnp.arange(NUM_EXPERTS)[None, None, :]).astype(jnp.float32)
    gate_vals = jnp.einsum('tke,te->tk', picked, router_prob)
    gate_f32 = w_gate.astype(jnp.float32)
    up_f32 = w_up.astype(jnp.float32)
    down_f32 = w_down.astype(jnp.float32)

    def block_step(acc_grads, blk_data):
        x_blk, dy_blk, top_blk, gate_blk = blk_data
        assign, is_valid, slot_pos = slot_tables(top_blk)
        src_tok = assign // TOP_K
        rows_x = jnp.where(is_valid[:, :, None], x_blk[src_tok], 0).astype(jnp.float32)
        slot_gate = jnp.where(is_valid, gate_blk.reshape(-1)[assign], 0.0)
        rows_g = (slot_gate[:, :, None] * dy_blk[src_tok].astype(jnp.float32)).astype(jnp.bfloat16).astype(jnp.float32)
        gate_pre = jnp.einsum('ecd,edf->ecf', rows_x, gate_f32)
        up_pre = jnp.einsum('ecd,edf->ecf', rows_x, up_f32)
        hidden = (jax.nn.silu(gate_pre) * up_pre).astype(jnp.bfloat16).astype(jnp.float32)
        out_rows = jnp.einsum('ecf,efd->ecd', hidden, down_f32).astype(jnp.bfloat16)
        d_hidden = jnp.einsum('ecd,efd->ecf', rows_g, down_f32)
        d_gate, d_up = silu_grads(d_hidden, gate_pre, up_pre)
        d_gate = d_gate.astype(jnp.float32)
        d_up = d_up.astype(jnp.float32)
        gw_gate = acc_grads[0] + jnp.einsum('ecd,ecf->edf', rows_x, d_gate)
        gw_up = acc_grads[1] + jnp.einsum('ecd,ecf->edf', rows_x, d_up)
        gw_down = acc_grads[2] + jnp.einsum('ecf,ecd->efd', hidden, rows_g)
        dx_rows = (jnp.einsum('ecf,edf->ecd', d_gate, gate_f32) + jnp.einsum('ecf,edf->ecd', d_up, up_f32)).astype(jnp.bfloat16)
        out_tok = out_rows.reshape(-1, MODEL_DIM)[slot_pos].reshape(TOK_DEV, TOP_K, MODEL_DIM).astype(jnp.float32)
        dx_tok = dx_rows.reshape(-1, MODEL_DIM)[slot_pos].reshape(TOK_DEV, TOP_K, MODEL_DIM).astype(jnp.float32)
        routed = jnp.sum(gate_blk[:, :, None] * out_tok, axis=1)
        gate_grad = jnp.einsum('td,tkd->tk', dy_blk.astype(jnp.float32), out_tok)
        dx_routed = jnp.sum(dx_tok, axis=1)
        return (gw_gate, gw_up, gw_down), (routed, gate_grad, dx_routed)

    zero_gate = jnp.zeros((NUM_EXPERTS, MODEL_DIM, EXPERT_FF), jnp.float32)
    zero_down = jnp.zeros((NUM_EXPERTS, EXPERT_FF, MODEL_DIM), jnp.float32)
    blk_inputs = (x_in.reshape(NUM_BLOCKS, TOK_DEV, MODEL_DIM), dy_in.reshape(NUM_BLOCKS, TOK_DEV, MODEL_DIM), top_ids.reshape(NUM_BLOCKS, TOK_DEV, TOP_K), gate_vals.reshape(NUM_BLOCKS, TOK_DEV, TOP_K))
    grads_out, per_blk = lax.scan(block_step, (zero_gate, zero_gate, zero_down), blk_inputs)
    routed = per_blk[0].reshape(TOKENS, MODEL_DIM)
    gate_grad = per_blk[1].reshape(TOKENS, TOP_K)
    dx_routed = per_blk[2].reshape(TOKENS, MODEL_DIM)

    sg_pre = jnp.dot(x_in, s_gate, preferred_element_type=jnp.float32)
    su_pre = jnp.dot(x_in, s_up, preferred_element_type=jnp.float32)
    s_hidden = (jax.nn.silu(sg_pre) * su_pre).astype(jnp.bfloat16)
    s_out = jnp.dot(s_hidden, s_down, preferred_element_type=jnp.float32)
    y_out = (routed + s_out).astype(jnp.bfloat16)

    d_prob = jnp.einsum('tke,tk->te', picked, gate_grad)
    d_logit = (router_prob * (d_prob - jnp.sum(router_prob * d_prob, axis=-1, keepdims=True))).astype(jnp.bfloat16)
    dw_router = jnp.dot(x_in.T, d_logit, preferred_element_type=jnp.float32)
    dx_router = jnp.dot(d_logit, w_router.T, preferred_element_type=jnp.float32)
    ds_hidden = jnp.dot(dy_in, s_down.T, preferred_element_type=jnp.float32)
    ds_gate_pre, ds_up_pre = silu_grads(ds_hidden, sg_pre, su_pre)
    ds_down = jnp.dot(s_hidden.T, dy_in, preferred_element_type=jnp.float32)
    ds_gate = jnp.dot(x_in.T, ds_gate_pre, preferred_element_type=jnp.float32)
    ds_up = jnp.dot(x_in.T, ds_up_pre, preferred_element_type=jnp.float32)
    dx_shared = jnp.dot(ds_gate_pre, s_gate.T, preferred_element_type=jnp.float32) + jnp.dot(ds_up_pre, s_up.T, preferred_element_type=jnp.float32)
    dx_out = (dx_routed + dx_shared + dx_router).astype(jnp.bfloat16)
    return (y_out, dx_out, dw_router, grads_out[0], grads_out[1], grads_out[2], ds_gate, ds_up, ds_down)
```

```python
import functools
import jax
import jax.numpy as jnp
from jax import lax
from jax.experimental import pallas as pl
from jax.experimental.pallas import tpu as pltpu
from jax.sharding import PartitionSpec as P

F32 = jnp.float32
BF16 = jnp.bfloat16
CHUNKS = 4
GROUP = 8


def silu_grads(d_hidden, gate_pre, up_pre):
    sig_gate = jax.nn.sigmoid(gate_pre)
    silu_gate = gate_pre * sig_gate
    d_gate = (d_hidden * up_pre * sig_gate * (1.0 + gate_pre * (1.0 - sig_gate))).astype(BF16)
    d_up = (d_hidden * silu_gate).astype(BF16)
    return d_gate, d_up


def combine_kernel(num_parts, per_part, slot_cap, weighted, first_blk, cnt_ref, tok_ref, gate_ref, *refs):
    parts, out_ref, buf = refs[:num_parts], refs[num_parts], refs[num_parts + 1]
    blk, exp = pl.program_id(0), pl.program_id(1)
    group_id = (blk + first_blk) * (num_parts * per_part) + exp

    @pl.when(exp == 0)
    def _():
        out_ref[...] = jnp.zeros_like(out_ref)

    for part in range(num_parts):
        @pl.when(exp // per_part == part)
        def _(part=part):
            buf[...] = parts[part][0, 0].astype(F32)

    count = cnt_ref[group_id]
    base = group_id * slot_cap

    def add_rows(first, num):
        toks = [tok_ref[base + first + u] for u in range(num)]
        rows = []
        for u in range(num):
            row = buf[pl.ds(first + u, 1), :]
            if weighted:
                row = row * gate_ref[base + first + u]
            rows.append(out_ref[0, pl.ds(toks[u], 1), :] + row)
        for u in range(num):
            out_ref[0, pl.ds(toks[u], 1), :] = rows[u]

    def full_step(i, carry):
        add_rows(i * GROUP, GROUP)
        return carry

    def tail_step(i, carry):
        add_rows(i, 1)
        return carry

    full = count // GROUP
    lax.fori_loop(0, full, full_step, 0)
    lax.fori_loop(full * GROUP, count, tail_step, 0)


def combine(parts, counts, toks, gates, tok_count, weighted, first, blocks):
    num_parts = len(parts)
    per_part, _, slot_cap, dim = parts[0].shape

    def part_map(part, b, e, *_):
        return (jnp.clip(e - part * per_part, 0, per_part - 1), b + first, 0, 0)

    return pl.pallas_call(
        functools.partial(combine_kernel, num_parts, per_part, slot_cap, weighted, first),
        grid_spec=pltpu.PrefetchScalarGridSpec(
            num_scalar_prefetch=3,
            grid=(blocks, num_parts * per_part),
            in_specs=[pl.BlockSpec((1, 1, slot_cap, dim), functools.partial(part_map, part)) for part in range(num_parts)],
            out_specs=pl.BlockSpec((1, tok_count, dim), lambda b, e, *_: (b, 0, 0)),
            scratch_shapes=[pltpu.VMEM((slot_cap, dim), F32)],
        ),
        out_shape=jax.ShapeDtypeStruct((blocks, tok_count, dim), F32),
        compiler_params=pltpu.CompilerParams(
            dimension_semantics=("arbitrary", "arbitrary"), vmem_limit_bytes=56 * 1024 * 1024),
        cost_estimate=pl.CostEstimate(flops=20_000_000_000, bytes_accessed=130_000_000, transcendentals=0),
    )(counts, toks, gates, *parts)


def solution(mesh):
    all_axes = ('dp', 'ep')
    ep_size = mesh.shape['ep']
    row_spec = P(all_axes, None)
    expert_spec = P('ep', 'dp', None)
    swap_chip = [(i, i ^ 2) for i in range(ep_size)]
    swap_core = [(i, i ^ 1) for i in range(ep_size)]
    swap_both = [(i, i ^ 3) for i in range(ep_size)]
    swap_dp = [(0, 1), (1, 0)]

    def spread(val):
        chip_val = lax.ppermute(val, 'ep', swap_chip)
        core_val = lax.ppermute(val, 'ep', swap_core)
        both_val = lax.ppermute(chip_val, 'ep', swap_core)
        return lax.optimization_barrier(jnp.stack([val, chip_val, core_val, both_val]))

    def collect(near, far):
        recv = lax.ppermute(far, 'ep', swap_core)
        return near[0] + recv[0] + lax.ppermute(near[1] + recv[1], 'ep', swap_chip)

    def local_step(x_loc, dy_loc, top_loc, wr_loc, wg_loc, wu_loc, wd_loc, sg_loc, su_loc, sd_loc):
        tok_count, top_k = top_loc.shape
        num_experts = wr_loc.shape[1]
        local_experts = num_experts // ep_size
        per_chunk = local_experts // CHUNKS
        slot_cap = 2 * tok_count * top_k // num_experts
        dp_idx = lax.axis_index('dp')
        ep_idx = lax.axis_index('ep')

        def gather_dp(shard):
            recv = lax.ppermute(shard, 'dp', swap_dp)
            return jnp.where(dp_idx == 0, jnp.concatenate([shard, recv], axis=1), jnp.concatenate([recv, shard], axis=1))

        def split_dp(full):
            half = full.shape[1] // 2
            return lax.dynamic_slice_in_dim(full, (1 - dp_idx) * half, half, axis=1), lax.dynamic_slice_in_dim(full, dp_idx * half, half, axis=1)

        shards = [[w[ci * per_chunk:(ci + 1) * per_chunk] for w in (wd_loc, wg_loc, wu_loc)] for ci in range(CHUNKS)]
        shards, x_loc, dy_loc, top_loc, wr_loc = lax.optimization_barrier((shards, x_loc, dy_loc, top_loc, wr_loc))
        chunk_w = [[gather_dp(w) for w in shards[ci]] for ci in range(CHUNKS)]

        x_all = spread(x_loc)
        dy_all = spread(dy_loc)
        w_router = lax.all_gather(wr_loc, all_axes, axis=0, tiled=True)
        s_gate = lax.all_gather(sg_loc, all_axes, axis=0, tiled=True)
        s_up = lax.all_gather(su_loc, all_axes, axis=0, tiled=True)
        s_down = lax.all_gather(sd_loc, all_axes, axis=0, tiled=True)

        logits = jnp.dot(x_loc, w_router, preferred_element_type=F32)
        router_prob = jax.nn.softmax(logits, axis=-1)
        picked = jnp.any(top_loc[:, :, None] == jnp.arange(num_experts)[None, None, :], axis=1)
        tok_ids = jnp.arange(tok_count)
        before = (tok_ids[None, :] < tok_ids[:, None]).astype(BF16)
        rank = jnp.dot(before, picked.astype(BF16), preferred_element_type=F32)
        slot_of = jnp.where(picked, rank, -1.0).T
        slot_ids = jnp.arange(slot_cap, dtype=F32)
        at_slot = slot_of[:, None, :] == slot_ids[None, :, None]
        tok_tab = jnp.sum(jnp.where(at_slot, (tok_ids + 1).astype(F32)[None, None, :], 0.0), axis=-1) - 1.0
        gate_tab = jnp.sum(jnp.where(at_slot, router_prob.T[:, None, :], 0.0), axis=-1)
        tabs = spread(jnp.stack([tok_tab, gate_tab]))
        tabs = lax.dynamic_slice_in_dim(tabs, ep_idx * local_experts, local_experts, axis=2)
        toks = tabs[:, 0].astype(jnp.int32)
        gates = tabs[:, 1]

        sg_pre = jnp.dot(x_loc, s_gate, preferred_element_type=F32)
        su_pre = jnp.dot(x_loc, s_up, preferred_element_type=F32)
        s_hidden = (jax.nn.silu(sg_pre) * su_pre).astype(BF16)
        s_out = jnp.dot(s_hidden, s_down, preferred_element_type=F32)
        ds_hidden = jnp.einsum('td,fd->tf', dy_loc, s_down, preferred_element_type=F32)
        ds_gate_pre, ds_up_pre = silu_grads(ds_hidden, sg_pre, su_pre)
        gs_down = jnp.einsum('tf,td->fd', s_hidden, dy_loc, preferred_element_type=F32)
        gs_gate = jnp.einsum('td,tf->df', x_loc, ds_gate_pre, preferred_element_type=F32)
        gs_up = jnp.einsum('td,tf->df', x_loc, ds_up_pre, preferred_element_type=F32)
        dx_shared = jnp.einsum('tf,df->td', ds_gate_pre, s_gate, preferred_element_type=F32) + jnp.einsum('tf,df->td', ds_up_pre, s_up, preferred_element_type=F32)

        toks, gs_gate, gs_up, gs_down, dx_shared, s_out = lax.optimization_barrier((toks, gs_gate, gs_up, gs_down, dx_shared, s_out))
        gs_gate, gs_up, gs_down = [lax.psum_scatter(g, all_axes, scatter_dimension=0, tiled=True) for g in (gs_gate, gs_up, gs_down)]
        out_parts, dx_parts, q_parts = [], [], []
        grads = []
        for ci in range(CHUNKS):
            w_down, w_gate, w_up = chunk_w[ci]
            sl = slice(ci * per_chunk, (ci + 1) * per_chunk)
            tok_c, gate_c = toks[:, sl], gates[:, sl]
            pick = (tok_c[..., None] == tok_ids).astype(BF16)
            rows_x = jnp.einsum('bect,btd->becd', pick, x_all, preferred_element_type=F32).astype(BF16)
            rows_dy = jnp.einsum('bect,btd->becd', pick, dy_all, preferred_element_type=F32).astype(BF16)
            rows_g = (gate_c[..., None] * rows_dy).astype(BF16)
            gate_pre = jnp.einsum('becd,edf->ebcf', rows_x, w_gate, preferred_element_type=F32)
            up_pre = jnp.einsum('becd,edf->ebcf', rows_x, w_up, preferred_element_type=F32)
            hidden = (jax.nn.silu(gate_pre) * up_pre).astype(BF16)
            out_rows = jnp.einsum('ebcf,efd->ebcd', hidden, w_down, preferred_element_type=F32).astype(BF16)
            q_parts.append(jnp.einsum('becd,ebcd->bec', rows_dy, out_rows, preferred_element_type=F32))
            d_hidden = jnp.einsum('becd,efd->ebcf', rows_g, w_down, preferred_element_type=F32)
            d_gate, d_up = silu_grads(d_hidden, gate_pre, up_pre)
            sent_down, kept_down = split_dp(jnp.einsum('ebcf,becd->efd', hidden, rows_g, preferred_element_type=F32))
            sent_gate, kept_gate = split_dp(jnp.einsum('becd,ebcf->edf', rows_x, d_gate, preferred_element_type=F32))
            sent_up, kept_up = split_dp(jnp.einsum('becd,ebcf->edf', rows_x, d_up, preferred_element_type=F32))
            dx_rows = (jnp.einsum('ebcf,edf->ebcd', d_gate, w_gate, preferred_element_type=F32) + jnp.einsum('ebcf,edf->ebcd', d_up, w_up, preferred_element_type=F32)).astype(BF16)
            toks, sent_down, sent_gate, sent_up, out_rows, dx_rows = lax.optimization_barrier((toks, sent_down, sent_gate, sent_up, out_rows, dx_rows))
            if ci == CHUNKS - 2:
                toks, gs_gate, gs_up, gs_down = lax.optimization_barrier((toks, gs_gate, gs_up, gs_down))
            recvs = [lax.ppermute(val, 'dp', swap_dp) for val in (sent_down, sent_gate, sent_up)]
            grads.append(([kept_down, kept_gate, kept_up], recvs))
            out_parts.append(out_rows)
            dx_parts.append(dx_rows)

        counts = jnp.sum((toks >= 0).astype(jnp.int32), axis=-1).reshape(-1)
        safe_toks = jnp.maximum(toks, 0).reshape(-1)
        flat_gates = gates.reshape(-1)
        near_cnt = ep_size // 2

        def join(parts, weighted):
            far = combine(parts, counts, safe_toks, flat_gates, tok_count, weighted, near_cnt, ep_size - near_cnt)
            near = combine(parts, counts, safe_toks, flat_gates, tok_count, weighted, 0, near_cnt)
            return collect(near, far)

        y_loc = (join(out_parts, True) + s_out).astype(BF16)
        dx_routed = join(dx_parts, False)

        q_tab = jnp.concatenate(q_parts, axis=1)
        q_from = [q_tab[0], lax.ppermute(q_tab[1], 'ep', swap_chip), lax.ppermute(q_tab[2], 'ep', swap_core), lax.ppermute(q_tab[3], 'ep', swap_both)]
        q_all = jnp.zeros((num_experts, slot_cap), F32)
        for rel, q_blk in zip((0, 2, 1, 3), q_from):
            q_all = lax.dynamic_update_slice_in_dim(q_all, q_blk, (ep_idx ^ rel) * local_experts, axis=0)
        d_prob = jnp.sum(jnp.where(at_slot, q_all[:, :, None], 0.0), axis=1).T
        d_logit = (router_prob * (d_prob - jnp.sum(router_prob * d_prob, axis=-1, keepdims=True))).astype(BF16)
        gw_router = jnp.einsum('td,te->de', x_loc, d_logit, preferred_element_type=F32)
        dx_router = jnp.einsum('te,de->td', d_logit, w_router, preferred_element_type=F32)
        dx_loc = (dx_routed + dx_shared + dx_router).astype(BF16)
        grads[-1][0][:], y_loc, dx_loc = lax.optimization_barrier((grads[-1][0], y_loc, dx_loc))
        totals = [jnp.zeros(w.shape, F32) for w in (wd_loc, wg_loc, wu_loc)]
        for ci, (kept, recvs) in enumerate(grads):
            totals = [lax.dynamic_update_slice(tot, k + r, (ci * per_chunk, 0, 0)) for tot, k, r in zip(totals, kept, recvs)]
        gw_down, gw_gate, gw_up = totals
        return (y_loc, dx_loc,
                lax.psum_scatter(gw_router, all_axes, scatter_dimension=0, tiled=True),
                gw_gate, gw_up, gw_down, gs_gate, gs_up, gs_down)

    return jax.shard_map(local_step, mesh=mesh,
                         in_specs=(row_spec, row_spec, row_spec, row_spec, expert_spec, expert_spec, expert_spec, row_spec, row_spec, row_spec),
                         out_specs=(row_spec, row_spec, row_spec, expert_spec, expert_spec, expert_spec, row_spec, row_spec, row_spec),
                         check_vma=False)
```

```python
import functools
import jax
import jax.numpy as jnp
from jax import lax
from jax.experimental import pallas as pl
from jax.experimental.pallas import tpu as pltpu
from jax.sharding import PartitionSpec as P

F32 = jnp.float32
BF16 = jnp.bfloat16
CHUNKS = 4
GROUP = 8


def silu_grads(d_hidden, gate_pre, up_pre):
    sig_gate = jax.nn.sigmoid(gate_pre)
    silu_gate = gate_pre * sig_gate
    d_gate = (d_hidden * up_pre * sig_gate * (1.0 + gate_pre * (1.0 - sig_gate))).astype(BF16)
    d_up = (d_hidden * silu_gate).astype(BF16)
    return d_gate, d_up


def combine_kernel(num_parts, per_part, slot_cap, weighted, first_blk, cnt_ref, tok_ref, gate_ref, *refs):
    parts, out_ref, buf = refs[:num_parts], refs[num_parts], refs[num_parts + 1]
    blk, exp = pl.program_id(0), pl.program_id(1)
    group_id = (blk + first_blk) * (num_parts * per_part) + exp

    @pl.when(exp == 0)
    def _():
        out_ref[...] = jnp.zeros_like(out_ref)

    for part in range(num_parts):
        @pl.when(exp // per_part == part)
        def _(part=part):
            buf[...] = parts[part][0, 0].astype(F32)

    count = cnt_ref[group_id]
    base = group_id * slot_cap

    def add_rows(first, num):
        toks = [tok_ref[base + first + u] for u in range(num)]
        rows = []
        for u in range(num):
            row = buf[pl.ds(first + u, 1), :]
            if weighted:
                row = row * gate_ref[base + first + u]
            rows.append(out_ref[0, pl.ds(toks[u], 1), :] + row)
        for u in range(num):
            out_ref[0, pl.ds(toks[u], 1), :] = rows[u]

    def full_step(i, carry):
        add_rows(i * GROUP, GROUP)
        return carry

    def tail_step(i, carry):
        add_rows(i, 1)
        return carry

    full = count // GROUP
    lax.fori_loop(0, full, full_step, 0)
    lax.fori_loop(full * GROUP, count, tail_step, 0)


def combine(parts, counts, toks, gates, tok_count, weighted, first, blocks):
    num_parts = len(parts)
    per_part, _, slot_cap, dim = parts[0].shape

    def part_map(part, b, e, *_):
        return (jnp.clip(e - part * per_part, 0, per_part - 1), b + first, 0, 0)

    return pl.pallas_call(
        functools.partial(combine_kernel, num_parts, per_part, slot_cap, weighted, first),
        grid_spec=pltpu.PrefetchScalarGridSpec(
            num_scalar_prefetch=3,
            grid=(blocks, num_parts * per_part),
            in_specs=[pl.BlockSpec((1, 1, slot_cap, dim), functools.partial(part_map, part)) for part in range(num_parts)],
            out_specs=pl.BlockSpec((1, tok_count, dim), lambda b, e, *_: (b, 0, 0)),
            scratch_shapes=[pltpu.VMEM((slot_cap, dim), F32)],
        ),
        out_shape=jax.ShapeDtypeStruct((blocks, tok_count, dim), F32),
        compiler_params=pltpu.CompilerParams(
            dimension_semantics=("arbitrary", "arbitrary"), vmem_limit_bytes=56 * 1024 * 1024),
        cost_estimate=pl.CostEstimate(flops=20_000_000_000, bytes_accessed=130_000_000, transcendentals=0),
    )(counts, toks, gates, *parts)


def solution(mesh):
    all_axes = ('dp', 'ep')
    ep_size = mesh.shape['ep']
    row_spec = P(all_axes, None)
    expert_spec = P('ep', 'dp', None)
    swap_chip = [(i, i ^ 2) for i in range(ep_size)]
    swap_core = [(i, i ^ 1) for i in range(ep_size)]
    swap_both = [(i, i ^ 3) for i in range(ep_size)]
    swap_dp = [(0, 1), (1, 0)]

    def spread(val):
        chip_val = lax.ppermute(val, 'ep', swap_chip)
        core_val = lax.ppermute(val, 'ep', swap_core)
        both_val = lax.ppermute(chip_val, 'ep', swap_core)
        return lax.optimization_barrier(jnp.stack([val, chip_val, core_val, both_val]))

    def local_step(x_loc, dy_loc, top_loc, wr_loc, wg_loc, wu_loc, wd_loc, sg_loc, su_loc, sd_loc):
        tok_count, top_k = top_loc.shape
        num_experts = wr_loc.shape[1]
        local_experts = num_experts // ep_size
        per_chunk = local_experts // CHUNKS
        slot_cap = 2 * tok_count * top_k // num_experts
        dp_idx = lax.axis_index('dp')
        ep_idx = lax.axis_index('ep')

        def gather_dp(shard):
            recv = lax.ppermute(shard, 'dp', swap_dp)
            return jnp.where(dp_idx == 0, jnp.concatenate([shard, recv], axis=1), jnp.concatenate([recv, shard], axis=1))

        def split_dp(full):
            half = full.shape[1] // 2
            return lax.dynamic_slice_in_dim(full, (1 - dp_idx) * half, half, axis=1), lax.dynamic_slice_in_dim(full, dp_idx * half, half, axis=1)

        shards = [[w[ci * per_chunk:(ci + 1) * per_chunk] for w in (wd_loc, wg_loc, wu_loc)] for ci in range(CHUNKS)]
        w_router = lax.all_gather(wr_loc, all_axes, axis=0, tiled=True)
        shards, x_loc, dy_loc, top_loc, w_router = lax.optimization_barrier((shards, x_loc, dy_loc, top_loc, w_router))
        chunk_w = [[gather_dp(w) for w in shards[ci]] for ci in range(CHUNKS)]

        x_all = spread(x_loc)
        dy_all = spread(dy_loc)
        s_gate = lax.all_gather(sg_loc, all_axes, axis=0, tiled=True)
        s_up = lax.all_gather(su_loc, all_axes, axis=0, tiled=True)
        s_down = lax.all_gather(sd_loc, all_axes, axis=0, tiled=True)

        logits = jnp.dot(x_loc, w_router, preferred_element_type=F32)
        router_prob = jax.nn.softmax(logits, axis=-1)
        picked = jnp.any(top_loc[:, :, None] == jnp.arange(num_experts)[None, None, :], axis=1)
        tok_ids = jnp.arange(tok_count)
        before = (tok_ids[None, :] < tok_ids[:, None]).astype(BF16)
        rank = jnp.dot(before, picked.astype(BF16), preferred_element_type=F32)
        slot_of = jnp.where(picked, rank, -1.0).T
        slot_ids = jnp.arange(slot_cap, dtype=F32)
        at_slot = slot_of[:, None, :] == slot_ids[None, :, None]
        tok_tab = jnp.sum(jnp.where(at_slot, (tok_ids + 1).astype(F32)[None, None, :], 0.0), axis=-1) - 1.0
        gate_tab = jnp.sum(jnp.where(at_slot, router_prob.T[:, None, :], 0.0), axis=-1)
        tabs = spread(jnp.stack([tok_tab, gate_tab]))
        tabs = lax.dynamic_slice_in_dim(tabs, ep_idx * local_experts, local_experts, axis=2)
        toks = tabs[:, 0].astype(jnp.int32)
        gates = tabs[:, 1]

        sg_pre = jnp.dot(x_loc, s_gate, preferred_element_type=F32)
        su_pre = jnp.dot(x_loc, s_up, preferred_element_type=F32)
        s_hidden = (jax.nn.silu(sg_pre) * su_pre).astype(BF16)
        s_out = jnp.dot(s_hidden, s_down, preferred_element_type=F32)
        ds_hidden = jnp.einsum('td,fd->tf', dy_loc, s_down, preferred_element_type=F32)
        ds_gate_pre, ds_up_pre = silu_grads(ds_hidden, sg_pre, su_pre)
        gs_down = jnp.einsum('tf,td->fd', s_hidden, dy_loc, preferred_element_type=F32)
        gs_gate = jnp.einsum('td,tf->df', x_loc, ds_gate_pre, preferred_element_type=F32)
        gs_up = jnp.einsum('td,tf->df', x_loc, ds_up_pre, preferred_element_type=F32)
        dx_shared = jnp.einsum('tf,df->td', ds_gate_pre, s_gate, preferred_element_type=F32) + jnp.einsum('tf,df->td', ds_up_pre, s_up, preferred_element_type=F32)

        toks, gs_gate, gs_up, gs_down, dx_shared, s_out = lax.optimization_barrier((toks, gs_gate, gs_up, gs_down, dx_shared, s_out))
        gs_gate, gs_up, gs_down = [lax.psum_scatter(g, all_axes, scatter_dimension=0, tiled=True) for g in (gs_gate, gs_up, gs_down)]
        counts = jnp.sum((toks >= 0).astype(jnp.int32), axis=-1).reshape(-1)
        safe_toks = jnp.maximum(toks, 0).reshape(-1)
        flat_gates = gates.reshape(-1)
        near_cnt = ep_size // 2

        def collect(parts, weighted):
            far = combine(parts, counts, safe_toks, flat_gates, tok_count, weighted, near_cnt, ep_size - near_cnt)
            near = combine(parts, counts, safe_toks, flat_gates, tok_count, weighted, 0, near_cnt)
            recv = lax.ppermute(far, 'ep', swap_core)
            return near[0] + recv[0], near[1] + recv[1]

        out_parts, dx_parts, q_parts = [], [], []
        grads = []
        for ci in range(CHUNKS):
            w_down, w_gate, w_up = chunk_w[ci]
            sl = slice(ci * per_chunk, (ci + 1) * per_chunk)
            tok_c, gate_c = toks[:, sl], gates[:, sl]
            pick = (tok_c[..., None] == tok_ids).astype(BF16)
            rows_x = jnp.einsum('bect,btd->becd', pick, x_all, preferred_element_type=F32).astype(BF16)
            rows_dy = jnp.einsum('bect,btd->becd', pick, dy_all, preferred_element_type=F32).astype(BF16)
            rows_g = (gate_c[..., None] * rows_dy).astype(BF16)
            gate_pre = jnp.einsum('becd,edf->ebcf', rows_x, w_gate, preferred_element_type=F32)
            up_pre = jnp.einsum('becd,edf->ebcf', rows_x, w_up, preferred_element_type=F32)
            hidden = (jax.nn.silu(gate_pre) * up_pre).astype(BF16)
            out_rows = jnp.einsum('ebcf,efd->ebcd', hidden, w_down, preferred_element_type=F32).astype(BF16)
            q_parts.append(jnp.einsum('becd,ebcd->bec', rows_dy, out_rows, preferred_element_type=F32))
            out_parts.append(out_rows)
            if ci == CHUNKS - 1:
                y_near, y_pass = collect(out_parts, True)
                rows_g, y_pass = lax.optimization_barrier((rows_g, y_pass))
                y_across = lax.ppermute(y_pass, 'ep', swap_chip)
            d_hidden = jnp.einsum('becd,efd->ebcf', rows_g, w_down, preferred_element_type=F32)
            d_gate, d_up = silu_grads(d_hidden, gate_pre, up_pre)
            sent_down, kept_down = split_dp(jnp.einsum('ebcf,becd->efd', hidden, rows_g, preferred_element_type=F32))
            sent_gate, kept_gate = split_dp(jnp.einsum('becd,ebcf->edf', rows_x, d_gate, preferred_element_type=F32))
            sent_up, kept_up = split_dp(jnp.einsum('becd,ebcf->edf', rows_x, d_up, preferred_element_type=F32))
            dx_rows = (jnp.einsum('ebcf,edf->ebcd', d_gate, w_gate, preferred_element_type=F32) + jnp.einsum('ebcf,edf->ebcd', d_up, w_up, preferred_element_type=F32)).astype(BF16)
            toks, sent_down, sent_gate, sent_up, dx_rows = lax.optimization_barrier((toks, sent_down, sent_gate, sent_up, dx_rows))
            if ci == CHUNKS - 2:
                toks, gs_gate, gs_up, gs_down = lax.optimization_barrier((toks, gs_gate, gs_up, gs_down))
            recvs = [lax.ppermute(val, 'dp', swap_dp) for val in (sent_down, sent_gate, sent_up)]
            grads.append(([kept_down, kept_gate, kept_up], recvs))
            dx_parts.append(dx_rows)

        dx_near, dx_pass = collect(dx_parts, False)
        dx_routed = dx_near + lax.ppermute(dx_pass, 'ep', swap_chip)
        y_loc = (y_near + y_across + s_out).astype(BF16)

        q_tab = jnp.concatenate(q_parts, axis=1)
        q_from = [q_tab[0], lax.ppermute(q_tab[1], 'ep', swap_chip), lax.ppermute(q_tab[2], 'ep', swap_core), lax.ppermute(q_tab[3], 'ep', swap_both)]
        q_all = jnp.zeros((num_experts, slot_cap), F32)
        for rel, q_blk in zip((0, 2, 1, 3), q_from):
            q_all = lax.dynamic_update_slice_in_dim(q_all, q_blk, (ep_idx ^ rel) * local_experts, axis=0)
        d_prob = jnp.sum(jnp.where(at_slot, q_all[:, :, None], 0.0), axis=1).T
        d_logit = (router_prob * (d_prob - jnp.sum(router_prob * d_prob, axis=-1, keepdims=True))).astype(BF16)
        gw_router = jnp.einsum('td,te->de', x_loc, d_logit, preferred_element_type=F32)
        dx_router = jnp.einsum('te,de->td', d_logit, w_router, preferred_element_type=F32)
        dx_loc = (dx_routed + dx_shared + dx_router).astype(BF16)
        grads[-1][0][:], y_loc, dx_loc = lax.optimization_barrier((grads[-1][0], y_loc, dx_loc))
        totals = [jnp.zeros(w.shape, F32) for w in (wd_loc, wg_loc, wu_loc)]
        for ci, (kept, recvs) in enumerate(grads):
            totals = [lax.dynamic_update_slice(tot, k + r, (ci * per_chunk, 0, 0)) for tot, k, r in zip(totals, kept, recvs)]
        gw_down, gw_gate, gw_up = totals
        return (y_loc, dx_loc,
                lax.psum_scatter(gw_router, all_axes, scatter_dimension=0, tiled=True),
                gw_gate, gw_up, gw_down, gs_gate, gs_up, gs_down)

    return jax.shard_map(local_step, mesh=mesh,
                         in_specs=(row_spec, row_spec, row_spec, row_spec, expert_spec, expert_spec, expert_spec, row_spec, row_spec, row_spec),
                         out_specs=(row_spec, row_spec, row_spec, expert_spec, expert_spec, expert_spec, row_spec, row_spec, row_spec),
                         check_vma=False)
```
